512 devices in a mesh: gx: 8 (over y), gy: 8 (over x, core), gz: 8 (over z).
Axes of the slice: x: 4, y: 8, z: 8, core: 2. Of those that a mesh axis runs over, the one named last changes fastest.
Arguments:
- wavefunctions: bfloat16 [128, 128, 128, 128], P('gx', 'gy', 'gz'), may hold values from -512 to 512, as said below
- potential: float32 [128, 128, 128], P('gx', 'gy', 'gz'), may hold values from 0 to 3
Outputs:
- rotated: float32 [128, 128, 128, 128], P('gx', 'gy', 'gz')
- residual: bfloat16 [128, 128, 128, 128], P('gx', 'gy', 'gz')
- quotients: float32 [128], replicated
- norms: float32 [128], replicated
The draws below stay inside these ranges and needn't reach their ends.
Inputs may be any that keep to these rules, and one draw needn't show every extreme that they name: `wavefunctions`: real values mixed across bands, of full rank.
All inputs are finite; a program needn't handle non-finite values.
Results may differ from the reference program's by a relative error of at most 0.0007.
Values may be sent and summed in bfloat16 or wider, within the bound.
No kernel may reach another device: no remote copies, remote signals or barrier semaphores. Data moves between devices by JAX's collectives and lax.ppermute only.
A program may use at most 64 MiB of HBM per device.

```python
import jax
import jax.numpy as jnp
from jax import lax

BANDS = 128
NX = 128
NY = 128
NZ = 128


def draw_wavefunctions(key, part):
    first, second, third = jax.random.split(jax.random.fold_in(key, 17), 3)
    values = jnp.clip(jax.random.normal(first, (NX, NY, NZ, BANDS), jnp.float32), -4.0, 4.0)
    scales = jnp.exp(jax.random.uniform(third, (BANDS,), jnp.float32, jnp.log(0.3), jnp.log(3.0)))
    mixing = jnp.eye(BANDS, dtype=jnp.float32) + 0.4 * jnp.clip(jax.random.normal(second, (BANDS, BANDS), jnp.float32), -3.0, 3.0) / jnp.sqrt(BANDS * 1.0)
    mixed = jnp.einsum('xyzb,bc->xyzc', values, mixing) * scales
    along_x = jnp.arange(NX, dtype=jnp.float32) / NX
    along_y = jnp.arange(NY, dtype=jnp.float32) / NY
    along_z = jnp.arange(NZ, dtype=jnp.float32) / NZ
    envelope = 0.5 * jnp.exp(0.55 * (along_x[:, None, None] + along_y[None, :, None] + along_z[None, None, :]))
    return (mixed * envelope[..., None]).astype(jnp.bfloat16)


def level_of(key, extent, cuts, smallest, high):
    factor_of, own = 1.0, jax.random.fold_in(key, 6)
    for axis_at, parts in cuts:
        steps = jnp.exp(jax.random.uniform(jax.random.fold_in(own, axis_at), (parts,), jnp.float32, smallest / len(cuts), high / len(cuts)))
        factor_of = factor_of * jnp.repeat(steps, extent[axis_at] // parts).reshape([-1 if axis == axis_at else 1 for axis in range(len(extent))])
    return factor_of


def setup_inputs(seed: int = 0) -> dict:
    key_list = jax.random.split(jax.random.key(seed), 3)
    wavefunctions = draw_wavefunctions(jax.random.fold_in(key_list[2], 71), 0)
    potential = jnp.clip(3.0 * jax.random.uniform(key_list[1], (NX, NY, NZ), jnp.float32) ** level_of(key_list[1], (NX, NY, NZ), ((0, 8), (1, 8), (2, 8)), -0.2, 0.2), 0.0, 3.0)
    return {"wavefunctions": wavefunctions, "potential": potential}


def kinetic(field):
    total = jnp.zeros_like(field)
    for axis in range(3):
        total = total + (-jnp.roll(field, 2, axis) + 16.0 * jnp.roll(field, 1, axis) - 30.0 * field + 16.0 * jnp.roll(field, -1, axis) - jnp.roll(field, -2, axis)) / 12.0
    return -0.5 * total

def reference(wavefunctions, potential):
    cells = NX * NY * NZ
    flat = wavefunctions.reshape(cells, BANDS)
    correlation = lax.dot_general(flat.astype(jnp.float32), flat.astype(jnp.float32), (((0,), (0,)), ((), ())), preferred_element_type=jnp.float32) / cells
    factor = jnp.linalg.cholesky(correlation)
    inverse = lax.linalg.triangular_solve(factor, jnp.eye(BANDS, dtype=jnp.float32), left_side=True, lower=True)
    rotated = jnp.dot(flat.astype(jnp.float32), inverse.T, precision=lax.Precision.HIGHEST).reshape(NX, NY, NZ, BANDS)
    width = BANDS // 8
    pieces, quotient_list, norm_list = ([], [], [])
    for block in range(8):
        part = rotated[..., block * width:(block + 1) * width]
        applied = kinetic(part) + potential[..., None] * part
        quotient = lax.optimization_barrier(jnp.sum(part * applied, axis=(0, 1, 2))) / cells
        leftover = applied - quotient * part
        norm_value = jnp.sqrt(lax.optimization_barrier(jnp.sum(leftover * leftover, axis=(0, 1, 2))) / cells + 1e-06)
        pieces.append(leftover.astype(jnp.bfloat16))
        quotient_list.append(quotient)
        norm_list.append(norm_value)
    residual = jnp.concatenate(pieces, axis=3)
    return (rotated, residual, jnp.concatenate(quotient_list), jnp.concatenate(norm_list))
```

```python
import functools

import jax
import jax.numpy as jnp
import numpy as np
from jax import lax
from jax.experimental import pallas as pl
from jax.experimental.pallas import tpu as pltpu
from jax.sharding import Mesh
from jax.sharding import PartitionSpec as P

GX = ("gx",)
GY = ("gy_0", "gy_1")
GZ = ("gz",)
NEAR = ("gy_0", "gz")
FAR = ("gx", "gy_1")
HIGHEST = lax.Precision.HIGHEST
CHUNKS = 4


def plane_weights(cy, cz):
    side = {0: 90.0, 1: -16.0, 2: 1.0}
    weights = np.zeros((cy * cz, cy * cz + 4 * cz + 4 * cy), np.float32)
    for y in range(cy):
        for z in range(cz):
            row = y * cz + z
            weights[row, row] = side[0]
            for step in (-2, -1, 1, 2):
                w = side[abs(step)]
                base = cy * cz
                if 0 <= y + step < cy:
                    weights[row, row + step * cz] = w
                elif y + step < 0:
                    weights[row, base + (y + step + 2) * cz + z] = w
                else:
                    weights[row, base + 2 * cz + (y + step - cy) * cz + z] = w
                base = cy * cz + 4 * cz
                if 0 <= z + step < cz:
                    weights[row, row + step] = w
                elif z + step < 0:
                    weights[row, base + y * 2 + z + step + 2] = w
                else:
                    weights[row, base + 2 * cy + y * 2 + z + step - cz] = w
    return weights


def over_cells(left, right):
    return lax.dot_general(
        left, right, (((0,), (0,)), ((), ())), preferred_element_type=jnp.float32
    )


def iotas(rows, columns):
    shape = (rows, columns)
    return lax.broadcasted_iota(jnp.int32, shape, 0), lax.broadcasted_iota(jnp.int32, shape, 1)


def apply_kernel(p, xlo, xhi, ylo, yhi, zlo, zhi, pot, weights, high, low, sums):
    cx, cells, bands = p.shape
    stencil = weights[...]
    total = None
    for x in range(cx):
        def plane(at):
            ref, at = (xlo, at + 2) if at < 0 else (xhi, at - cx) if at >= cx else (p, at)
            return ref[at].astype(jnp.float32)

        own = p[x]
        around = jnp.concatenate([own, ylo[x], yhi[x], zlo[x], zhi[x]], axis=0)
        kinetic = jnp.dot(stencil, around, preferred_element_type=jnp.float32)
        kinetic = kinetic + (plane(x - 2) + plane(x + 2)) - 16.0 * (plane(x - 1) + plane(x + 1))
        given = own.astype(jnp.float32)
        applied = kinetic * (1.0 / 24.0) + pot[:, x : x + 1] * given
        top = applied.astype(jnp.bfloat16)
        rest = (applied - top.astype(jnp.float32)).astype(jnp.bfloat16)
        high[x] = top
        low[x] = rest
        part = over_cells(
            jnp.concatenate([own, top], axis=1), jnp.concatenate([own, top, rest], axis=1)
        )
        total = part if total is None else total + part
    b = bands
    row, column = iotas(b, b)
    gram = total[:b, :b]
    cross = total[:b, b : 2 * b] + total[:b, 2 * b :]
    rest = total[b:, 2 * b :]
    square = total[b:, b : 2 * b] + rest + rest.T
    cross_own = jnp.sum(jnp.where(row == column, cross, 0.0), axis=0, keepdims=True)
    cross = cross + cross.T
    sums[:b] = jnp.where(row >= column, gram, cross)
    spare = jnp.where(row == 0, cross_own, pltpu.roll(jnp.broadcast_to(cross_own, (b, b)), b - 1, 1))
    sums[b:] = jnp.where(row > column, 2.0 * square, jnp.where(row == column, square, spare))


def across(value, lane):
    return jnp.broadcast_to(value[:, lane : lane + 1], value.shape)


def down(value, row):
    return jnp.broadcast_to(value[row : row + 1, :], value.shape)


def inverse_factor(rows):
    count = len(rows)
    size, bands = rows[0].shape
    row, column = iotas(size, bands)
    rows = list(rows)
    right = [jnp.where(column == row + size * k, 1.0, 0.0) for k in range(count)]
    done = []
    for k in range(count):
        own = [across(rows[k], size * k + c) for c in range(size)]
        below = {
            i: [across(rows[i], size * k + c) for c in range(size)] for i in range(k + 1, count)
        }
        left_k, right_k = rows[k], right[k]
        result = jnp.zeros_like(right_k)
        pivots = []
        for c in range(size):
            pivot = down(own[c], c)
            share = 1.0 / pivot
            left_row, right_row = down(left_k, c), down(right_k, c)
            pivots.append((left_row, right_row))
            result = jnp.where(row == c, right_row * lax.rsqrt(pivot), result)
            factor = jnp.where(row > c, own[c] * share, 0.0)
            left_k = left_k - factor * left_row
            right_k = right_k - factor * right_row
            entries = [down(own[d], c) for d in range(c + 1, size)]
            for d, entry in zip(range(c + 1, size), entries):
                own[d] = own[d] - factor * entry
            for lines in below.values():
                lines[c] = lines[c] * share
                for d, entry in zip(range(c + 1, size), entries):
                    lines[d] = lines[d] - lines[c] * entry
        done.append(result)
        for i, lines in below.items():
            for line, (left_row, right_row) in zip(lines, pivots):
                rows[i] = rows[i] - line * left_row
                right[i] = right[i] - line * right_row
    return done


def split_3(value):
    parts = []
    for _ in range(3):
        part = value.astype(jnp.bfloat16)
        value = value - part.astype(jnp.float32)
        parts.append(part)
    return parts


def finish_kernel(
    cells, sums, p, high, low, rotated, residual, quotients, norms, w, w_low, out_r, out_s, sems
):
    rows, bands = p.shape
    row, column = iotas(bands, bands)
    scale = 1.0 / cells
    first, second = sums[:bands] * scale, sums[bands:] * scale
    lower = jnp.where(row >= column, first, 0.0)
    gram = lower + jnp.where(row > column, first, 0.0).T
    own = jnp.where(column[:1] == 0, pltpu.roll(second[:8], 1, 1)[1:2], second[:1])
    cross = jnp.where(row < column, first, jnp.where(row == column, own, 0.0))
    square = jnp.where(row >= column, second, 0.0)
    size = 8
    inverse = jnp.concatenate(
        inverse_factor([gram[i : i + size] for i in range(0, bands, size)]), axis=0
    )

    def diagonal(matrix):
        product = jnp.dot(inverse, matrix, precision=HIGHEST, preferred_element_type=jnp.float32)
        return jnp.sum(product * inverse, axis=1, keepdims=True)

    quotient = diagonal(cross)
    squares = diagonal(square) - quotient * quotient * (2.0 - diagonal(gram))
    norm = jnp.sqrt(jnp.maximum(squares, 0.0) + 1e-06)
    quotients[...] = jnp.broadcast_to(quotient, (bands, bands)).T[:8]
    norms[...] = jnp.broadcast_to(norm, (bands, bands)).T[:8]

    turned = inverse.T
    shifted = (-quotient * inverse).T
    none = jnp.zeros((bands, bands), jnp.bfloat16)
    for at, (a, s) in enumerate(zip(split_3(turned), split_3(shifted))):
        w[at, :bands, :bands] = a
        w[at, :bands, bands:] = s
        w[at, bands:, :bands] = none
        w[at, bands:, bands:] = a
        if at < 2:
            w_low[at * bands : (at + 1) * bands] = a
    step = rows // CHUNKS
    copies = []
    for chunk in range(CHUNKS):
        part = pl.ds(chunk * step, step)
        both = jnp.concatenate([p[part], high[part]], axis=1)
        rest = low[part]
        result = jnp.dot(both, w[2], preferred_element_type=jnp.float32)
        result = result + jnp.dot(both, w[1], preferred_element_type=jnp.float32)
        result = result + jnp.dot(both, w[0], preferred_element_type=jnp.float32)
        extra = jnp.dot(
            jnp.concatenate([rest, rest], axis=1), w_low[...], preferred_element_type=jnp.float32
        )
        out_r[part] = result[:, :bands]
        out_s[part] = (result[:, bands:] + extra).astype(jnp.bfloat16)
        for at, (source, target) in enumerate(((out_r, rotated), (out_s, residual))):
            copy = pltpu.make_async_copy(source.at[part], target.at[part], sems.at[chunk, at])
            copy.start()
            copies.append(copy)
    for copy in copies:
        copy.wait()


def vmem(count):
    return [pl.BlockSpec(memory_space=pltpu.VMEM)] * count


def from_neighbours(low_edge, high_edge, axes):
    count = lax.axis_size(axes)
    up = [(i, (i + 1) % count) for i in range(count)]
    return (
        lax.ppermute(high_edge, axes, up),
        lax.ppermute(low_edge, axes, [(b, a) for a, b in up]),
    )


def exchange(blocks, axes):
    return lax.all_to_all(blocks, axes, split_axis=0, concat_axis=0, tiled=True)


def for_each(value, axes):
    return exchange(jnp.broadcast_to(value, (lax.axis_size(axes), *value.shape)), axes)


def sum_everywhere(value):
    rows, columns = value.shape
    own = jnp.sum(exchange(value.reshape(lax.axis_size(NEAR), -1, columns), NEAR), axis=0)
    own = jnp.sum(for_each(own, FAR), axis=0)
    return for_each(own, NEAR).reshape(rows, columns)


def local(wavefunctions, potential):
    cx, cy, cz, bands = wavefunctions.shape
    cells = cx * cy * cz
    total_cells = cells * lax.axis_size(GX) * lax.axis_size(GY) * lax.axis_size(GZ)
    planes = wavefunctions.reshape(cx, cy * cz, bands)
    ylo, yhi = from_neighbours(
        wavefunctions[:, :2].reshape(cx, 2 * cz, bands),
        wavefunctions[:, cy - 2 :].reshape(cx, 2 * cz, bands),
        GY,
    )
    xlo, xhi = from_neighbours(planes[:2], planes[cx - 2 :], GX)
    zlo, zhi = from_neighbours(
        wavefunctions[:, :, :2].reshape(cx, 2 * cy, bands),
        wavefunctions[:, :, cz - 2 :].reshape(cx, 2 * cy, bands),
        GZ,
    )
    weights = jnp.asarray(plane_weights(cy, cz), jnp.bfloat16)
    shape = (cx, cy * cz, bands)
    high, low, sums = pl.pallas_call(
        apply_kernel,
        out_shape=(
            jax.ShapeDtypeStruct(shape, jnp.bfloat16),
            jax.ShapeDtypeStruct(shape, jnp.bfloat16),
            jax.ShapeDtypeStruct((2 * bands, bands), jnp.float32),
        ),
        in_specs=vmem(9),
        out_specs=tuple(vmem(3)),
        name="apply",
    )(planes, xlo, xhi, ylo, yhi, zlo, zhi, potential.reshape(cx, cy * cz).T, weights)
    sums = sum_everywhere(sums)
    flat = (cells, bands)
    kept = pl.BlockSpec(memory_space=pl.ANY)
    rotated, residual, quotients, norms = pl.pallas_call(
        functools.partial(finish_kernel, total_cells),
        out_shape=(
            jax.ShapeDtypeStruct(flat, jnp.float32),
            jax.ShapeDtypeStruct(flat, jnp.bfloat16),
            jax.ShapeDtypeStruct((8, bands), jnp.float32),
            jax.ShapeDtypeStruct((8, bands), jnp.float32),
        ),
        in_specs=vmem(4),
        out_specs=(kept, kept, *vmem(2)),
        scratch_shapes=[
            pltpu.VMEM((3, 2 * bands, 2 * bands), jnp.bfloat16),
            pltpu.VMEM((2 * bands, bands), jnp.bfloat16),
            pltpu.VMEM(flat, jnp.float32),
            pltpu.VMEM(flat, jnp.bfloat16),
            pltpu.SemaphoreType.DMA((CHUNKS, 2)),
        ],
        name="finish",
    )(sums, planes.reshape(flat), high.reshape(flat), low.reshape(flat))
    whole = (cx, cy, cz, bands)
    return rotated.reshape(whole), residual.reshape(whole), quotients[0], norms[0]


def solution(mesh):
    torus = Mesh(
        mesh.devices.reshape(mesh.shape["gx"], 4, 2, mesh.shape["gz"]), ("gx", "gy_0", "gy_1", "gz")
    )
    return jax.shard_map(
        local,
        mesh=torus,
        in_specs=(P("gx", GY, "gz", None), P("gx", GY, "gz")),
        out_specs=(P("gx", GY, "gz", None), P("gx", GY, "gz", None), P(), P()),
        check_vma=False,
    )
```

```python
import functools

import jax
import jax.numpy as jnp
import numpy as np
from jax import lax
from jax.experimental import pallas as pl
from jax.experimental.pallas import tpu as pltpu
from jax.sharding import Mesh
from jax.sharding import PartitionSpec as P

GX = ("gx_0", "gx_1")
GY = ("gy_0", "gy_1")
GZ = ("gz_0", "gz_1")
NEAR = ("gy_0", "gy_1", "gx_1", "gz_1")
FAR = ("gx_0", "gz_0")
HIGHEST = lax.Precision.HIGHEST
CHUNKS = 4
VMEM_LIMIT = 24 * 2**20


def plane_weights(cy, cz):
    side = {0: 90.0, 1: -16.0, 2: 1.0}
    weights = np.zeros((cy * cz, cy * cz + 4 * cz + 4 * cy), np.float32)
    for y in range(cy):
        for z in range(cz):
            row = y * cz + z
            weights[row, row] = side[0]
            for step in (-2, -1, 1, 2):
                w = side[abs(step)]
                base = cy * cz
                if 0 <= y + step < cy:
                    weights[row, row + step * cz] = w
                elif y + step < 0:
                    weights[row, base + (y + step + 2) * cz + z] = w
                else:
                    weights[row, base + 2 * cz + (y + step - cy) * cz + z] = w
                base = cy * cz + 4 * cz
                if 0 <= z + step < cz:
                    weights[row, row + step] = w
                elif z + step < 0:
                    weights[row, base + y * 2 + z + step + 2] = w
                else:
                    weights[row, base + 2 * cy + y * 2 + z + step - cz] = w
    return weights


def over_cells(left, right):
    return lax.dot_general(
        left, right, (((0,), (0,)), ((), ())), preferred_element_type=jnp.float32
    )


def iotas(rows, columns):
    shape = (rows, columns)
    return lax.broadcasted_iota(jnp.int32, shape, 0), lax.broadcasted_iota(jnp.int32, shape, 1)


def apply_kernel(p, xlo, xhi, ylo, yhi, zlo, zhi, pot, weights, high, low, sums, total):
    cx, cells, bands = p.shape
    cy, cz = pot.shape[1:]
    b = bands

    def plane(at):
        if isinstance(at, int) and not 0 <= at < cx:
            return (xlo[at + 2] if at < 0 else xhi[at - cx]).astype(jnp.float32)
        return p[at].astype(jnp.float32)

    def slab(x):
        own = p[x]
        around = jnp.concatenate([own, ylo[x], yhi[x], zlo[x], zhi[x]], axis=0)
        kinetic = jnp.dot(weights[...], around, preferred_element_type=jnp.float32)
        kinetic = kinetic + (plane(x - 2) + plane(x + 2)) - 16.0 * (plane(x - 1) + plane(x + 1))
        lines = pot[x].T
        given = jnp.concatenate(
            [jnp.broadcast_to(lines[:, y : y + 1], (cz, b)) for y in range(cy)], axis=0
        ) * own.astype(jnp.float32)
        applied = kinetic * (1.0 / 24.0) + given
        top = applied.astype(jnp.bfloat16)
        rest = (applied - top.astype(jnp.float32)).astype(jnp.bfloat16)
        high[x] = top
        low[x] = rest
        return over_cells(
            jnp.concatenate([own, top], axis=1), jnp.concatenate([own, top, rest], axis=1)
        )

    total[...] = slab(0) + slab(1) + slab(cx - 2) + slab(cx - 1)

    def two_more(i, carry):
        x = 2 + 2 * i
        total[...] += slab(x) + slab(x + 1)
        return carry

    lax.fori_loop(0, (cx - 4) // 2, two_more, 0)
    row, column = iotas(b, b)
    gram = total[:b, :b]
    cross = total[:b, b : 2 * b] + total[:b, 2 * b :]
    rest = total[b:, 2 * b :]
    square = total[b:, b : 2 * b] + rest + rest.T
    cross_own = jnp.sum(jnp.where(row == column, cross, 0.0), axis=0, keepdims=True)
    cross = cross + cross.T
    sums[:b] = jnp.where(row >= column, gram, cross)
    spare = jnp.where(row == 0, cross_own, pltpu.roll(jnp.broadcast_to(cross_own, (b, b)), b - 1, 1))
    sums[b:] = jnp.where(row > column, 2.0 * square, jnp.where(row == column, square, spare))


def across(value, lane):
    return jnp.broadcast_to(value[:, lane : lane + 1], value.shape)


def down(value, row):
    return jnp.broadcast_to(value[row : row + 1, :], value.shape)


def inverse_factor(rows):
    count = len(rows)
    size, bands = rows[0].shape
    row, column = iotas(size, bands)
    rows = list(rows)
    right = [jnp.where(column == row + size * k, 1.0, 0.0) for k in range(count)]
    done = []
    for k in range(count):
        own = [across(rows[k], size * k + c) for c in range(size)]
        below = {
            i: [across(rows[i], size * k + c) for c in range(size)] for i in range(k + 1, count)
        }
        left_k, right_k = rows[k], right[k]
        result = jnp.zeros_like(right_k)
        pivots = []
        for c in range(size):
            pivot = down(own[c], c)
            share = 1.0 / pivot
            left_row, right_row = down(left_k, c), down(right_k, c)
            pivots.append((left_row, right_row))
            result = jnp.where(row == c, right_row * lax.rsqrt(pivot), result)
            factor = jnp.where(row > c, own[c] * share, 0.0)
            left_k = left_k - factor * left_row
            right_k = right_k - factor * right_row
            entries = [down(own[d], c) for d in range(c + 1, size)]
            for d, entry in zip(range(c + 1, size), entries):
                own[d] = own[d] - factor * entry
            for lines in below.values():
                lines[c] = lines[c] * share
                for d, entry in zip(range(c + 1, size), entries):
                    lines[d] = lines[d] - lines[c] * entry
        done.append(result)
        for i, lines in below.items():
            for line, (left_row, right_row) in zip(lines, pivots):
                rows[i] = rows[i] - line * left_row
                right[i] = right[i] - line * right_row
    return done


def split_3(value):
    parts = []
    for _ in range(3):
        part = value.astype(jnp.bfloat16)
        value = value - part.astype(jnp.float32)
        parts.append(part)
    return parts


def finish_kernel(
    cells, sums, p, high, low, rotated, residual, quotients, norms, w, w_low, out_r, out_s, sems
):
    rows, bands = p.shape
    row, column = iotas(bands, bands)
    scale = 1.0 / cells
    first, second = sums[:bands] * scale, sums[bands:] * scale
    lower = jnp.where(row >= column, first, 0.0)
    gram = lower + jnp.where(row > column, first, 0.0).T
    own = jnp.where(column[:1] == 0, pltpu.roll(second[:8], 1, 1)[1:2], second[:1])
    cross = jnp.where(row < column, first, jnp.where(row == column, own, 0.0))
    square = jnp.where(row >= column, second, 0.0)
    size = 8
    inverse = jnp.concatenate(
        inverse_factor([gram[i : i + size] for i in range(0, bands, size)]), axis=0
    )

    def diagonal(matrix):
        product = jnp.dot(inverse, matrix, precision=HIGHEST, preferred_element_type=jnp.float32)
        return jnp.sum(product * inverse, axis=1, keepdims=True)

    quotient = diagonal(cross)
    squares = diagonal(square) - quotient * quotient * (2.0 - diagonal(gram))
    norm = jnp.sqrt(jnp.maximum(squares, 0.0) + 1e-06)
    quotients[...] = jnp.broadcast_to(quotient, (bands, bands)).T[:1]
    norms[...] = jnp.broadcast_to(norm, (bands, bands)).T[:1]

    turned = inverse.T
    shifted = (-quotient * inverse).T
    none = jnp.zeros((bands, bands), jnp.bfloat16)
    for at, (a, s) in enumerate(zip(split_3(turned), split_3(shifted))):
        w[at, :bands, :bands] = a
        w[at, :bands, bands:] = s
        w[at, bands:, :bands] = none
        w[at, bands:, bands:] = a
        if at < 2:
            w_low[at * bands : (at + 1) * bands] = a
    step = rows // CHUNKS
    copies = []
    for chunk in range(CHUNKS):
        part = pl.ds(chunk * step, step)
        both = jnp.concatenate([p[part], high[part]], axis=1)
        rest = low[part]
        result = jnp.dot(both, w[2], preferred_element_type=jnp.float32)
        result = result + jnp.dot(both, w[1], preferred_element_type=jnp.float32)
        result = result + jnp.dot(both, w[0], preferred_element_type=jnp.float32)
        extra = jnp.dot(
            jnp.concatenate([rest, rest], axis=1), w_low[...], preferred_element_type=jnp.float32
        )
        out_r[part] = result[:, :bands]
        out_s[part] = (result[:, bands:] + extra).astype(jnp.bfloat16)
        for at, (source, target) in enumerate(((out_r, rotated), (out_s, residual))):
            copy = pltpu.make_async_copy(source.at[part], target.at[part], sems.at[chunk, at])
            copy.start()
            copies.append(copy)
    for copy in copies:
        copy.wait()


def near(value):
    return pltpu.with_memory_space_constraint(value, pltpu.VMEM)


def vmem(count):
    return [pl.BlockSpec(memory_space=pltpu.VMEM)] * count


def from_neighbours(low_edge, high_edge, axes):
    count = lax.axis_size(axes)
    up = [(i, (i + 1) % count) for i in range(count)]
    return (
        lax.ppermute(high_edge, axes, up),
        lax.ppermute(low_edge, axes, [(b, a) for a, b in up]),
    )


def exchange(blocks, axes):
    return lax.all_to_all(blocks, axes, split_axis=0, concat_axis=0, tiled=True)


def for_each(value, axes):
    return exchange(jnp.broadcast_to(value, (lax.axis_size(axes), *value.shape)), axes)


def sum_everywhere(value):
    rows, columns = value.shape
    own = jnp.sum(exchange(value.reshape(lax.axis_size(NEAR), -1, columns), NEAR), axis=0)
    own = jnp.sum(for_each(own, FAR), axis=0)
    return for_each(own, NEAR).reshape(rows, columns)


def local(wavefunctions, potential):
    cx, cy, cz, bands = wavefunctions.shape
    cells = cx * cy * cz
    total_cells = cells * lax.axis_size(GX) * lax.axis_size(GY) * lax.axis_size(GZ)
    planes = wavefunctions.reshape(cx, cy * cz, bands)
    ylo, yhi = from_neighbours(
        wavefunctions[:, :2].reshape(cx, 2 * cz, bands),
        wavefunctions[:, cy - 2 :].reshape(cx, 2 * cz, bands),
        GY,
    )
    xlo, xhi = from_neighbours(planes[:2], planes[cx - 2 :], GX)
    zlo, zhi = from_neighbours(
        wavefunctions[:, :, :2].reshape(cx, 2 * cy, bands),
        wavefunctions[:, :, cz - 2 :].reshape(cx, 2 * cy, bands),
        GZ,
    )
    weights = jnp.asarray(plane_weights(cy, cz), jnp.bfloat16)
    shape = (cx, cy * cz, bands)
    high, low, sums = pl.pallas_call(
        apply_kernel,
        out_shape=(
            pltpu.VMEM(shape, jnp.bfloat16),
            pltpu.VMEM(shape, jnp.bfloat16),
            pltpu.VMEM((2 * bands, bands), jnp.float32),
        ),
        in_specs=vmem(9),
        out_specs=tuple(vmem(3)),
        scratch_shapes=[pltpu.VMEM((2 * bands, 3 * bands), jnp.float32)],
        compiler_params=pltpu.CompilerParams(vmem_limit_bytes=VMEM_LIMIT),
        name="apply",
    )(*map(near, (planes, xlo, xhi, ylo, yhi, zlo, zhi, potential, weights)))
    sums = sum_everywhere(sums)
    flat = (cells, bands)
    kept = pl.BlockSpec(memory_space=pl.ANY)
    rotated, residual, quotients, norms = pl.pallas_call(
        functools.partial(finish_kernel, total_cells),
        out_shape=(
            jax.ShapeDtypeStruct(flat, jnp.float32),
            jax.ShapeDtypeStruct(flat, jnp.bfloat16),
            jax.ShapeDtypeStruct((1, bands), jnp.float32),
            jax.ShapeDtypeStruct((1, bands), jnp.float32),
        ),
        in_specs=vmem(4),
        out_specs=(kept, kept, *vmem(2)),
        scratch_shapes=[
            pltpu.VMEM((3, 2 * bands, 2 * bands), jnp.bfloat16),
            pltpu.VMEM((2 * bands, bands), jnp.bfloat16),
            pltpu.VMEM(flat, jnp.float32),
            pltpu.VMEM(flat, jnp.bfloat16),
            pltpu.SemaphoreType.DMA((CHUNKS, 2)),
        ],
        compiler_params=pltpu.CompilerParams(vmem_limit_bytes=VMEM_LIMIT),
        name="finish",
    )(*map(near, (sums, planes.reshape(flat), high.reshape(flat), low.reshape(flat))))
    whole = (cx, cy, cz, bands)
    return rotated.reshape(whole), residual.reshape(whole), quotients[0], norms[0]


def solution(mesh):
    count = mesh.shape
    torus = Mesh(
        mesh.devices.reshape(count["gx"] // 2, 2, count["gy"] // 2, 2, count["gz"] // 2, 2),
        GX + GY + GZ,
    )
    return jax.shard_map(
        local,
        mesh=torus,
        in_specs=(P(GX, GY, GZ, None), P(GX, GY, GZ)),
        out_specs=(P(GX, GY, GZ, None), P(GX, GY, GZ, None), P(), P()),
        check_vma=False,
    )
```

```python
import functools

import jax
import jax.numpy as jnp
import numpy as np
from jax import lax
from jax.experimental import pallas as pl
from jax.experimental.pallas import tpu as pltpu
from jax.sharding import Mesh
from jax.sharding import PartitionSpec as P

GX = ("gx_0", "gx_1")
GY = ("gy_0", "gy_1")
GZ = ("gz_0", "gz_1")
NEAR = ("gy_0", "gy_1", "gx_1", "gz_1")
FAR = ("gx_0", "gz_0")
HIGHEST = lax.Precision.HIGHEST
CHUNKS = 4
VMEM_LIMIT = 24 * 2**20


def plane_weights(cy, cz):
    side = {0: 90.0, 1: -16.0, 2: 1.0}
    weights = np.zeros((cy * cz, cy * cz + 4 * cz + 4 * cy), np.float32)
    for y in range(cy):
        for z in range(cz):
            row = y * cz + z
            weights[row, row] = side[0]
            for step in (-2, -1, 1, 2):
                w = side[abs(step)]
                base = cy * cz
                if 0 <= y + step < cy:
                    weights[row, row + step * cz] = w
                elif y + step < 0:
                    weights[row, base + (y + step + 2) * cz + z] = w
                else:
                    weights[row, base + 2 * cz + (y + step - cy) * cz + z] = w
                base = cy * cz + 4 * cz
                if 0 <= z + step < cz:
                    weights[row, row + step] = w
                elif z + step < 0:
                    weights[row, base + y * 2 + z + step + 2] = w
                else:
                    weights[row, base + 2 * cy + y * 2 + z + step - cz] = w
    return weights


def over_cells(left, right):
    return lax.dot_general(
        left, right, (((0,), (0,)), ((), ())), preferred_element_type=jnp.float32
    )


def iotas(rows, columns):
    shape = (rows, columns)
    return lax.broadcasted_iota(jnp.int32, shape, 0), lax.broadcasted_iota(jnp.int32, shape, 1)


def prepare_kernel(cy, given, potential, weights, p, xlo, xhi, ylo, yhi, zlo, zhi, pot, w, sems):
    cx, cells, bands = p.shape
    cz = cells // cy
    edge = 2 * cz
    pairs = (
        (given, p),
        (given.at[:2], xlo),
        (given.at[cx - 2 :], xhi),
        (given.at[:, :edge], ylo),
        (given.at[:, cells - edge :], yhi),
        (potential, pot),
        (weights, w),
    )
    copies = [pltpu.make_async_copy(*pair, sems.at[at]) for at, pair in enumerate(pairs)]
    for copy in copies:
        copy.start()
    row, column = iotas(4 * cy, cells)
    side, row = row // (2 * cy), row % (2 * cy)
    source = (row // 2) * cz + row % 2 + side * (cz - 2)
    choice = jnp.where(column == source, 1.0, 0.0).astype(jnp.bfloat16)
    copies[0].wait()
    for x in range(cx):
        faces = jnp.dot(choice, p[x], preferred_element_type=jnp.float32).astype(jnp.bfloat16)
        zlo[x] = faces[: 2 * cy]
        zhi[x] = faces[2 * cy :]
    for copy in copies[1:]:
        copy.wait()


def inner_kernel(p, pot, weights, inner):
    cx, cells, bands = p.shape
    cy, cz = pot.shape[1:]

    def slab(x, steps):
        own = p[x]
        total = jnp.dot(weights[:, :cells], own, preferred_element_type=jnp.float32)
        for step in steps:
            near_by = p[x + step].astype(jnp.float32)
            total = total + near_by if abs(step) == 2 else total - 16.0 * near_by
        lines = pot[x].T
        given = jnp.concatenate(
            [jnp.broadcast_to(lines[:, y : y + 1], (cz, bands)) for y in range(cy)], axis=0
        ) * own.astype(jnp.float32)
        inner[x] = total * (1.0 / 24.0) + given

    for x in range(cx):
        slab(x, [step for step in (-2, -1, 1, 2) if 0 <= x + step < cx])


def apply_kernel(p, inner, xlo, xhi, ylo, yhi, zlo, zhi, weights, high, low, sums):
    cx, cells, bands = p.shape
    b = bands

    def slab(x, outside=()):
        around = jnp.concatenate([ylo[x], yhi[x], zlo[x], zhi[x]], axis=0)
        missing = jnp.dot(weights[:, cells:], around, preferred_element_type=jnp.float32)
        for weight, ref, at in outside:
            missing = missing + weight * ref[at].astype(jnp.float32)
        applied = inner[x] + missing * (1.0 / 24.0)
        top = applied.astype(jnp.bfloat16)
        rest = (applied - top.astype(jnp.float32)).astype(jnp.bfloat16)
        high[x] = top
        low[x] = rest

    outside = {
        0: ((1.0, xlo, 0), (-16.0, xlo, 1)),
        1: ((1.0, xlo, 1),),
        cx - 2: ((1.0, xhi, 0),),
        cx - 1: ((-16.0, xhi, 0), (1.0, xhi, 1)),
    }
    for x in range(cx):
        slab(x, outside.get(x, ()))
    flat = [ref[...].reshape(cx * cells, b) for ref in (p, high, low)]
    total = over_cells(jnp.concatenate(flat[:2], axis=1), jnp.concatenate(flat, axis=1))
    row, column = iotas(b, b)
    gram = total[:b, :b]
    cross = total[:b, b : 2 * b] + total[:b, 2 * b :]
    rest = total[b:, 2 * b :]
    square = total[b:, b : 2 * b] + rest + rest.T
    cross_own = jnp.sum(jnp.where(row == column, cross, 0.0), axis=0, keepdims=True)
    cross = cross + cross.T
    sums[:b] = jnp.where(row >= column, gram, cross)
    spare = jnp.where(row == 0, cross_own, pltpu.roll(jnp.broadcast_to(cross_own, (b, b)), b - 1, 1))
    sums[b:] = jnp.where(row > column, 2.0 * square, jnp.where(row == column, square, spare))


def across(value, lane):
    return jnp.take_along_axis(value, jnp.full(value.shape, lane, jnp.int32), axis=1)


def down(value, row):
    return jnp.broadcast_to(value[row : row + 1, :], value.shape)


def inverse_factor(rows):
    count = len(rows)
    size, bands = rows[0].shape
    row, column = iotas(size, bands)
    rows = list(rows)
    right = [jnp.where(column == row + size * k, 1.0, 0.0) for k in range(count)]
    done = []
    for k in range(count):
        lines = {i: [] for i in range(k, count)}
        for c in range(size):
            for i in range(k, count):
                lines[i].append(across(rows[i], size * k + c))
        own = lines.pop(k) + [rows[k], right[k]]
        result = jnp.zeros_like(right[k])
        for c in range(size):
            here = row == c
            pivot = down(own[c], c)
            scale = lax.rsqrt(pivot)
            share = 1.0 / pivot
            factor = jnp.where(here, -1.0, own[c])
            result = jnp.where(here, own[-1] * scale, result)
            for d in range(c + 1, len(own)):
                own[d] = jnp.where(here, 0.0, own[d]) - factor * (down(own[d], c) * share)
        done.append(result)
        heads = [(down(own[-2], c), down(own[-1], c)) for c in range(size)]
        for i, line in lines.items():
            for at, (left_row, right_row) in zip(line, heads):
                rows[i] = rows[i] - at * left_row
                right[i] = right[i] - at * right_row
    return done


def split_3(value):
    parts = []
    for _ in range(3):
        part = value.astype(jnp.bfloat16)
        value = value - part.astype(jnp.float32)
        parts.append(part)
    return parts


def finish_kernel(
    cells, sums, p, high, low, rotated, residual, quotients, norms, w, out_r, out_s, sems
):
    rows, bands = p.shape
    row, column = iotas(bands, bands)
    scale = 1.0 / cells
    first, second = sums[:bands] * scale, sums[bands:] * scale
    lower = jnp.where(row >= column, first, 0.0)
    gram = lower + jnp.where(row > column, first, 0.0).T
    own = jnp.where(column[:1] == 0, pltpu.roll(second[:8], 1, 1)[1:2], second[:1])
    cross = jnp.where(row < column, first, jnp.where(row == column, own, 0.0))
    square = jnp.where(row >= column, second, 0.0)
    size = 8
    inverse = jnp.concatenate(
        inverse_factor([gram[i : i + size] for i in range(0, bands, size)]), axis=0
    )

    def diagonal(matrix):
        product = jnp.dot(inverse, matrix, precision=HIGHEST, preferred_element_type=jnp.float32)
        return jnp.sum(product * inverse, axis=1, keepdims=True)

    quotient = diagonal(cross)
    squares = diagonal(square) - quotient * quotient * (2.0 - diagonal(gram))
    norm = jnp.sqrt(jnp.maximum(squares, 0.0) + 1e-06)
    quotients[...] = jnp.broadcast_to(quotient, (bands, bands)).T[:1]
    norms[...] = jnp.broadcast_to(norm, (bands, bands)).T[:1]

    turned = inverse.T
    shifted = (-quotient * inverse).T
    none = jnp.zeros((bands, bands), jnp.bfloat16)
    for at, (a, s) in enumerate(zip(split_3(turned), split_3(shifted))):
        w[at, :bands, :bands] = a
        w[at, :bands, bands:] = s
        w[at, bands:, :bands] = none
        w[at, bands:, bands:] = a if at < 2 else w[0, bands:, bands:]
    step = rows // CHUNKS
    copies = []
    for chunk in range(CHUNKS):
        part = pl.ds(chunk * step, step)
        both = jnp.concatenate([p[part], high[part]], axis=1)
        rest = jnp.concatenate([p[part], low[part]], axis=1)
        result = jnp.dot(rest, w[2], preferred_element_type=jnp.float32)
        result = result + jnp.dot(both, w[1], preferred_element_type=jnp.float32)
        result = result + jnp.dot(both, w[0], preferred_element_type=jnp.float32)
        out_r[part] = result[:, :bands]
        out_s[part] = result[:, bands:].astype(jnp.bfloat16)
        for at, (source, target) in enumerate(((out_r, rotated), (out_s, residual))):
            copy = pltpu.make_async_copy(source.at[part], target.at[part], sems.at[chunk, at])
            copy.start()
            copies.append(copy)
    for copy in copies:
        copy.wait()


def near(value):
    return pltpu.with_memory_space_constraint(value, pltpu.VMEM)


def far(value):
    return pltpu.with_memory_space_constraint(value, pltpu.HBM)


def from_neighbours(low_edge, high_edge, axes):
    count = lax.axis_size(axes)
    up = [(i, (i + 1) % count) for i in range(count)]
    return (
        lax.ppermute(high_edge, axes, up),
        lax.ppermute(low_edge, axes, [(b, a) for a, b in up]),
    )


def kernel_call(kernel, outs, ins, outs_at, scratch=(), **kept):
    return pl.pallas_call(
        kernel,
        out_shape=outs,
        in_specs=[pl.BlockSpec(memory_space=space) for space in ins],
        out_specs=tuple(pl.BlockSpec(memory_space=space) for space in outs_at),
        scratch_shapes=scratch,
        compiler_params=pltpu.CompilerParams(vmem_limit_bytes=VMEM_LIMIT),
        **kept,
    )


def exchange(blocks, axes):
    return lax.all_to_all(blocks, axes, split_axis=0, concat_axis=0, tiled=True)


def for_each(value, axes):
    return exchange(jnp.broadcast_to(value, (lax.axis_size(axes), *value.shape)), axes)


def sum_everywhere(value):
    rows, columns = value.shape
    own = jnp.sum(exchange(value.reshape(lax.axis_size(NEAR), -1, columns), NEAR), axis=0)
    own = jnp.sum(for_each(own, FAR), axis=0)
    return for_each(own, NEAR).reshape(rows, columns)


def local(wavefunctions, potential):
    cx, cy, cz, bands = wavefunctions.shape
    cells = cx * cy * cz
    total_cells = cells * lax.axis_size(GX) * lax.axis_size(GY) * lax.axis_size(GZ)
    planes = wavefunctions.reshape(cx, cy * cz, bands)
    weights = jnp.asarray(plane_weights(cy, cz), jnp.bfloat16)
    shape = planes.shape
    on_chip, off_chip = pltpu.VMEM, pltpu.HBM

    def half(*dims):
        return on_chip(dims, jnp.bfloat16)

    p, *edges, pot, w = kernel_call(
        functools.partial(prepare_kernel, cy),
        (
            half(*shape),
            *[half(2, cy * cz, bands)] * 2,
            *[half(cx, 2 * cz, bands)] * 2,
            *[half(cx, 2 * cy, bands)] * 2,
            on_chip(potential.shape, jnp.float32),
            half(*weights.shape),
        ),
        [off_chip] * 3,
        [on_chip] * 9,
        [pltpu.SemaphoreType.DMA((7,))],
        name="prepare",
    )(*map(far, (planes, potential, weights)))
    xlo, xhi = from_neighbours(*edges[:2], GX)
    ylo, yhi = from_neighbours(*edges[2:4], GY)
    zlo, zhi = from_neighbours(*edges[4:], GZ)
    inner = kernel_call(
        inner_kernel, (on_chip(shape, jnp.float32),), [on_chip] * 3, [on_chip], name="inner"
    )(*map(near, (p, pot, w)))[0]
    high, low, sums = kernel_call(
        apply_kernel,
        (half(*shape), half(*shape), on_chip((2 * bands, bands), jnp.float32)),
        [on_chip] * 9,
        [on_chip] * 3,
        name="apply",
    )(*map(near, (p, inner, xlo, xhi, ylo, yhi, zlo, zhi, w)))
    sums = sum_everywhere(sums)
    flat = (cells, bands)
    line = jax.ShapeDtypeStruct((1, bands), jnp.float32)
    rotated, residual, quotients, norms = kernel_call(
        functools.partial(finish_kernel, total_cells),
        (
            jax.ShapeDtypeStruct(flat, jnp.float32),
            jax.ShapeDtypeStruct(flat, jnp.bfloat16),
            line,
            line,
        ),
        [on_chip] * 4,
        [off_chip, off_chip, on_chip, on_chip],
        [
            pltpu.VMEM((3, 2 * bands, 2 * bands), jnp.bfloat16),
            pltpu.VMEM(flat, jnp.float32),
            pltpu.VMEM(flat, jnp.bfloat16),
            pltpu.SemaphoreType.DMA((CHUNKS, 2)),
        ],
        name="finish",
    )(*map(near, (sums, p.reshape(flat), high.reshape(flat), low.reshape(flat))))
    whole = (cx, cy, cz, bands)
    return rotated.reshape(whole), residual.reshape(whole), quotients[0], norms[0]


def solution(mesh):
    count = mesh.shape
    torus = Mesh(
        mesh.devices.reshape(count["gx"] // 2, 2, count["gy"] // 2, 2, count["gz"] // 2, 2),
        GX + GY + GZ,
    )
    return jax.shard_map(
        local,
        mesh=torus,
        in_specs=(P(GX, GY, GZ, None), P(GX, GY, GZ)),
        out_specs=(P(GX, GY, GZ, None), P(GX, GY, GZ, None), P(), P()),
        check_vma=False,
    )
```

```python
import functools

import jax
import jax.numpy as jnp
import numpy as np
from jax import lax
from jax.experimental import pallas as pl
from jax.experimental.pallas import tpu as pltpu
from jax.sharding import Mesh
from jax.sharding import PartitionSpec as P

GX = ("gx_0", "gx_1")
GY = ("gy_0", "gy_1")
GZ = ("gz_0", "gz_1")
NEAR = ("gy_0", "gy_1", "gx_1", "gz_1")
FAR = ("gx_0", "gz_0")
HIGHEST = lax.Precision.HIGHEST
CHUNKS = (512,) * 8
VMEM_LIMIT = 24 * 2**20


def plane_weights(cy, cz):
    side = {0: 90.0, 1: -16.0, 2: 1.0}
    weights = np.zeros((cy * cz, cy * cz + 4 * cz + 4 * cy), np.float32)
    for y in range(cy):
        for z in range(cz):
            row = y * cz + z
            weights[row, row] = side[0]
            for step in (-2, -1, 1, 2):
                w = side[abs(step)]
                base = cy * cz
                if 0 <= y + step < cy:
                    weights[row, row + step * cz] = w
                elif y + step < 0:
                    weights[row, base + (y + step + 2) * cz + z] = w
                else:
                    weights[row, base + 2 * cz + (y + step - cy) * cz + z] = w
                base = cy * cz + 4 * cz
                if 0 <= z + step < cz:
                    weights[row, row + step] = w
                elif z + step < 0:
                    weights[row, base + y * 2 + z + step + 2] = w
                else:
                    weights[row, base + 2 * cy + y * 2 + z + step - cz] = w
    return weights


def over_cells(left, right):
    return lax.dot_general(
        left, right, (((0,), (0,)), ((), ())), preferred_element_type=jnp.float32
    )


def iotas(rows, columns):
    shape = (rows, columns)
    return lax.broadcasted_iota(jnp.int32, shape, 0), lax.broadcasted_iota(jnp.int32, shape, 1)


def prepare_kernel(cy, given, potential, weights, p, xlo, xhi, ylo, yhi, zlo, zhi, pot, w, sems):
    cx, cells, bands = p.shape
    cz = cells // cy
    edge = 2 * cz
    pairs = (
        (given, p),
        (given.at[:2], xlo),
        (given.at[cx - 2 :], xhi),
        (given.at[:, :edge], ylo),
        (given.at[:, cells - edge :], yhi),
        (potential, pot),
        (weights, w),
    )
    copies = [pltpu.make_async_copy(*pair, sems.at[at]) for at, pair in enumerate(pairs)]
    for copy in copies:
        copy.start()
    row, column = iotas(4 * cy, cells)
    side, row = row // (2 * cy), row % (2 * cy)
    source = (row // 2) * cz + row % 2 + side * (cz - 2)
    choice = jnp.where(column == source, 1.0, 0.0).astype(jnp.bfloat16)
    copies[0].wait()
    for x in range(cx):
        faces = jnp.dot(choice, p[x], preferred_element_type=jnp.float32).astype(jnp.bfloat16)
        zlo[x] = faces[: 2 * cy]
        zhi[x] = faces[2 * cy :]
    for copy in copies[1:]:
        copy.wait()


def inner_kernel(p, pot, weights, inner):
    cx, cells, bands = p.shape
    cy, cz = pot.shape[1:]

    def slab(x, steps):
        own = p[x]
        total = jnp.dot(weights[:, :cells], own, preferred_element_type=jnp.float32)
        for step in steps:
            near_by = p[x + step].astype(jnp.float32)
            total = total + near_by if abs(step) == 2 else total - 16.0 * near_by
        lines = pot[x].T
        given = jnp.concatenate(
            [jnp.broadcast_to(lines[:, y : y + 1], (cz, bands)) for y in range(cy)], axis=0
        ) * own.astype(jnp.float32)
        inner[x] = total * (1.0 / 24.0) + given

    for x in range(cx):
        slab(x, [step for step in (-2, -1, 1, 2) if 0 <= x + step < cx])


def apply_kernel(p, inner, ylo, yhi, xlo, zlo, xhi, zhi, weights, high, low, sums):
    cx, cells, bands = p.shape
    b = bands

    def slab(x, outside=()):
        around = jnp.concatenate([ylo[x], yhi[x], zlo[x], zhi[x]], axis=0)
        missing = jnp.dot(weights[:, cells:], around, preferred_element_type=jnp.float32)
        for weight, ref, at in outside:
            missing = missing + weight * ref[at].astype(jnp.float32)
        applied = inner[x] + missing * (1.0 / 24.0)
        top = applied.astype(jnp.bfloat16)
        rest = (applied - top.astype(jnp.float32)).astype(jnp.bfloat16)
        high[x] = top
        low[x] = rest

    outside = {
        0: ((1.0, xlo, 0), (-16.0, xlo, 1)),
        1: ((1.0, xlo, 1),),
        cx - 2: ((1.0, xhi, 0),),
        cx - 1: ((-16.0, xhi, 0), (1.0, xhi, 1)),
    }
    for x in range(cx):
        slab(x, outside.get(x, ()))
    flat = [ref[...].reshape(cx * cells, b) for ref in (p, high, low)]
    total = over_cells(jnp.concatenate(flat[:2], axis=1), jnp.concatenate(flat, axis=1))
    row, column = iotas(b, b)
    gram = total[:b, :b]
    cross = total[:b, b : 2 * b] + total[:b, 2 * b :]
    rest = total[b:, 2 * b :]
    square = total[b:, b : 2 * b] + rest + rest.T
    cross_own = jnp.sum(jnp.where(row == column, cross, 0.0), axis=0, keepdims=True)
    cross = cross + cross.T
    sums[:b] = jnp.where(row >= column, gram, cross)
    spare = jnp.where(row == 0, cross_own, pltpu.roll(jnp.broadcast_to(cross_own, (b, b)), b - 1, 1))
    sums[b:] = jnp.where(row > column, 2.0 * square, jnp.where(row == column, square, spare))


def across(value, lane):
    return jnp.take_along_axis(value, jnp.full(value.shape, lane, jnp.int32), axis=1)


def down(value, row):
    return jnp.broadcast_to(value[row : row + 1, :], value.shape)


def inverse_factor(rows):
    count = len(rows)
    size, bands = rows[0].shape
    row, column = iotas(size, bands)
    rows = list(rows)
    right = [jnp.where(column == row + size * k, 1.0, 0.0) for k in range(count)]
    done = []
    for k in range(count):
        lines = {
            i: [across(rows[i], size * k + c) for c in range(size)] for i in range(k, count)
        }
        own = lines.pop(k) + [rows[k], right[k]]
        result = jnp.zeros_like(right[k])
        for c in range(size):
            here = row == c
            pivot = down(own[c], c)
            scale = lax.rsqrt(pivot)
            share = 1.0 / pivot
            factor = jnp.where(here, -1.0, own[c])
            result = jnp.where(here, own[-1] * scale, result)
            for d in range(c + 1, len(own)):
                own[d] = jnp.where(here, 0.0, own[d]) - factor * (down(own[d], c) * share)
        done.append(result)
        heads = [(down(own[-2], c), down(own[-1], c)) for c in range(size)]
        for i, line in lines.items():
            for at in range(0, size, 2):
                rows[i] = rows[i] - (line[at] * heads[at][0] + line[at + 1] * heads[at + 1][0])
                right[i] = right[i] - (line[at] * heads[at][1] + line[at + 1] * heads[at + 1][1])
    return done


def split_3(value):
    parts = []
    for _ in range(3):
        part = value.astype(jnp.bfloat16)
        value = value - part.astype(jnp.float32)
        parts.append(part)
    return parts


def finish_kernel(
    cells, sums, p, high, low, rotated, residual, quotients, norms, w, out_r, out_s, sems
):
    bands = p.shape[1]
    row, column = iotas(bands, bands)
    scale = 1.0 / cells
    first, second = sums[:bands] * scale, sums[bands:] * scale
    lower = jnp.where(row >= column, first, 0.0)
    gram = lower + jnp.where(row > column, first, 0.0).T
    own = jnp.where(column[:1] == 0, pltpu.roll(second[:8], 1, 1)[1:2], second[:1])
    cross = jnp.where(row < column, first, jnp.where(row == column, own, 0.0))
    square = jnp.where(row >= column, second, 0.0)
    size = 16
    turned = jnp.concatenate(
        inverse_factor([gram[i : i + size] for i in range(0, bands, size)]), axis=0
    ).T
    none = jnp.zeros((bands, bands), jnp.bfloat16)
    for at, part in enumerate(split_3(turned)):
        w[at, :bands, :bands] = part
        w[at, :bands, bands:] = none
        w[at, bands:, :bands] = none
        w[at, bands:, bands:] = part if at < 2 else w[0, bands:, bands:]

    def diagonal(matrix):
        product = jnp.dot(matrix, turned, precision=HIGHEST, preferred_element_type=jnp.float32)
        return jnp.sum(product * turned, axis=0, keepdims=True)

    quotient = diagonal(cross)
    squares = diagonal(square) - quotient * quotient * (2.0 - diagonal(gram))
    quotients[...] = quotient
    norms[...] = jnp.sqrt(jnp.maximum(squares, 0.0) + 1e-06)
    copies = []
    start = 0
    for chunk, step in enumerate(CHUNKS):
        part = pl.ds(start, step)
        start += step
        both = jnp.concatenate([p[part], high[part]], axis=1)
        rest = jnp.concatenate([p[part], low[part]], axis=1)
        result = jnp.dot(rest, w[2], preferred_element_type=jnp.float32)
        result = result + jnp.dot(both, w[1], preferred_element_type=jnp.float32)
        result = result + jnp.dot(both, w[0], preferred_element_type=jnp.float32)
        bands_now = result[:, :bands]
        out_r[part] = bands_now
        out_s[part] = (result[:, bands:] - quotient * bands_now).astype(jnp.bfloat16)
        for at, (source, target) in enumerate(((out_r, rotated), (out_s, residual))):
            copy = pltpu.make_async_copy(source.at[part], target.at[part], sems.at[chunk, at])
            copy.start()
            copies.append(copy)
    for copy in copies:
        copy.wait()


def near(value):
    return pltpu.with_memory_space_constraint(value, pltpu.VMEM)


def far(value):
    return pltpu.with_memory_space_constraint(value, pltpu.HBM)


def from_below(edge, axes):
    count = lax.axis_size(axes)
    return lax.ppermute(edge, axes, [(i, (i + 1) % count) for i in range(count)])


def from_above(edge, axes):
    count = lax.axis_size(axes)
    return lax.ppermute(edge, axes, [((i + 1) % count, i) for i in range(count)])


def kernel_call(kernel, outs, ins, outs_at, scratch=(), **kept):
    return pl.pallas_call(
        kernel,
        out_shape=outs,
        in_specs=[pl.BlockSpec(memory_space=space) for space in ins],
        out_specs=tuple(pl.BlockSpec(memory_space=space) for space in outs_at),
        scratch_shapes=scratch,
        compiler_params=pltpu.CompilerParams(vmem_limit_bytes=VMEM_LIMIT),
        **kept,
    )


def exchange(blocks, axes):
    return lax.all_to_all(blocks, axes, split_axis=0, concat_axis=0, tiled=True)


def for_each(value, axes):
    return exchange(jnp.broadcast_to(value, (lax.axis_size(axes), *value.shape)), axes)


def sum_everywhere(value):
    rows, columns = value.shape
    own = jnp.sum(exchange(value.reshape(lax.axis_size(NEAR), -1, columns), NEAR), axis=0)
    own = jnp.sum(for_each(own, FAR), axis=0)
    return for_each(own, NEAR).reshape(rows, columns)


def local(wavefunctions, potential):
    cx, cy, cz, bands = wavefunctions.shape
    cells = cx * cy * cz
    total_cells = cells * lax.axis_size(GX) * lax.axis_size(GY) * lax.axis_size(GZ)
    planes = wavefunctions.reshape(cx, cy * cz, bands)
    weights = jnp.asarray(plane_weights(cy, cz), jnp.bfloat16)
    shape = planes.shape
    on_chip, off_chip = pltpu.VMEM, pltpu.HBM

    def half(*dims):
        return on_chip(dims, jnp.bfloat16)

    p, *edges, pot, w = kernel_call(
        functools.partial(prepare_kernel, cy),
        (
            half(*shape),
            *[half(2, cy * cz, bands)] * 2,
            *[half(cx, 2 * cz, bands)] * 2,
            *[half(cx, 2 * cy, bands)] * 2,
            on_chip(potential.shape, jnp.float32),
            half(*weights.shape),
        ),
        [off_chip] * 3,
        [on_chip] * 9,
        [pltpu.SemaphoreType.DMA((7,))],
        name="prepare",
    )(*map(far, (planes, potential, weights)))
    xlow, xhigh, ylow, yhigh, zlow, zhigh = edges
    ylo, yhi = from_below(yhigh, GY), from_above(ylow, GY)
    xlo, zlo = from_below(xhigh, GX), from_below(zhigh, GZ)
    xhi, zhi = from_above(xlow, GX), from_above(zlow, GZ)
    inner = kernel_call(
        inner_kernel, (on_chip(shape, jnp.float32),), [on_chip] * 3, [on_chip], name="inner"
    )(*map(near, (p, pot, w)))[0]
    high, low, sums = kernel_call(
        apply_kernel,
        (half(*shape), half(*shape), on_chip((2 * bands, bands), jnp.float32)),
        [on_chip] * 9,
        [on_chip] * 3,
        name="apply",
    )(*map(near, (p, inner, ylo, yhi, xlo, zlo, xhi, zhi, w)))
    sums = sum_everywhere(sums)
    flat = (cells, bands)
    line = jax.ShapeDtypeStruct((1, bands), jnp.float32)
    rotated, residual, quotients, norms = kernel_call(
        functools.partial(finish_kernel, total_cells),
        (
            jax.ShapeDtypeStruct(flat, jnp.float32),
            jax.ShapeDtypeStruct(flat, jnp.bfloat16),
            line,
            line,
        ),
        [on_chip] * 4,
        [off_chip, off_chip, on_chip, on_chip],
        [
            pltpu.VMEM((3, 2 * bands, 2 * bands), jnp.bfloat16),
            pltpu.VMEM(flat, jnp.float32),
            pltpu.VMEM(flat, jnp.bfloat16),
            pltpu.SemaphoreType.DMA((len(CHUNKS), 2)),
        ],
        name="finish",
    )(*map(near, (sums, p.reshape(flat), high.reshape(flat), low.reshape(flat))))
    whole = (cx, cy, cz, bands)
    return rotated.reshape(whole), residual.reshape(whole), quotients[0], norms[0]


def solution(mesh):
    count = mesh.shape
    torus = Mesh(
        mesh.devices.reshape(count["gx"] // 2, 2, count["gy"] // 2, 2, count["gz"] // 2, 2),
        GX + GY + GZ,
    )
    return jax.shard_map(
        local,
        mesh=torus,
        in_specs=(P(GX, GY, GZ, None), P(GX, GY, GZ)),
        out_specs=(P(GX, GY, GZ, None), P(GX, GY, GZ, None), P(), P()),
        check_vma=False,
    )
```

```python
import functools

import jax
import jax.numpy as jnp
import numpy as np
from jax import lax
from jax.experimental import pallas as pl
from jax.experimental.pallas import tpu as pltpu
from jax.sharding import Mesh
from jax.sharding import PartitionSpec as P

GX = ("gx_0", "gx_1")
GY = ("gy_0", "gy_1")
GZ = ("gz_0", "gz_1")
NEAR = ("gy_0", "gy_1", "gx_1", "gz_1")
FAR = ("gx_0", "gz_0")
HIGHEST = lax.Precision.HIGHEST
CHUNKS = (512,) * 8
VMEM_LIMIT = 24 * 2**20


def plane_weights(cy, cz):
    side = {0: 90.0, 1: -16.0, 2: 1.0}
    weights = np.zeros((cy * cz, cy * cz + 4 * cz + 4 * cy), np.float32)
    for y in range(cy):
        for z in range(cz):
            row = y * cz + z
            weights[row, row] = side[0]
            for step in (-2, -1, 1, 2):
                w = side[abs(step)]
                base = cy * cz
                if 0 <= y + step < cy:
                    weights[row, row + step * cz] = w
                elif y + step < 0:
                    weights[row, base + (y + step + 2) * cz + z] = w
                else:
                    weights[row, base + 2 * cz + (y + step - cy) * cz + z] = w
                base = cy * cz + 4 * cz
                if 0 <= z + step < cz:
                    weights[row, row + step] = w
                elif z + step < 0:
                    weights[row, base + y * 2 + z + step + 2] = w
                else:
                    weights[row, base + 2 * cy + y * 2 + z + step - cz] = w
    return weights


def over_cells(left, right):
    return lax.dot_general(
        left, right, (((0,), (0,)), ((), ())), preferred_element_type=jnp.float32
    )


def iotas(rows, columns):
    shape = (rows, columns)
    return lax.broadcasted_iota(jnp.int32, shape, 0), lax.broadcasted_iota(jnp.int32, shape, 1)


def prepare_kernel(cy, given, potential, weights, p, xlo, xhi, ylo, yhi, zlo, zhi, pot, w, sems):
    cx, cells, bands = p.shape
    cz = cells // cy
    edge = 2 * cz
    pairs = (
        (given, p),
        (given.at[:2], xlo),
        (given.at[cx - 2 :], xhi),
        (given.at[:, :edge], ylo),
        (given.at[:, cells - edge :], yhi),
        (potential, pot),
        (weights, w),
    )
    copies = [pltpu.make_async_copy(*pair, sems.at[at]) for at, pair in enumerate(pairs)]
    for copy in copies:
        copy.start()
    row, column = iotas(4 * cy, cells)
    side, row = row // (2 * cy), row % (2 * cy)
    source = (row // 2) * cz + row % 2 + side * (cz - 2)
    choice = jnp.where(column == source, 1.0, 0.0).astype(jnp.bfloat16)
    copies[0].wait()
    for x in range(cx):
        faces = jnp.dot(choice, p[x], preferred_element_type=jnp.float32).astype(jnp.bfloat16)
        zlo[x] = faces[: 2 * cy]
        zhi[x] = faces[2 * cy :]
    for copy in copies[1:]:
        copy.wait()


def inner_kernel(p, pot, weights, inner):
    cx, cells, bands = p.shape
    cy, cz = pot.shape[1:]

    def slab(x, steps):
        own = p[x]
        total = jnp.dot(weights[:, :cells], own, preferred_element_type=jnp.float32)
        for step in steps:
            near_by = p[x + step].astype(jnp.float32)
            total = total + near_by if abs(step) == 2 else total - 16.0 * near_by
        lines = pot[x].T
        given = jnp.concatenate(
            [jnp.broadcast_to(lines[:, y : y + 1], (cz, bands)) for y in range(cy)], axis=0
        ) * own.astype(jnp.float32)
        inner[x] = total * (1.0 / 24.0) + given

    for x in range(cx):
        slab(x, [step for step in (-2, -1, 1, 2) if 0 <= x + step < cx])


def apply_kernel(p, inner, xlo, xhi, zlo, zhi, ylo, yhi, weights, high, low, sums):
    cx, cells, bands = p.shape
    b = bands

    def slab(x, outside=()):
        around = jnp.concatenate([ylo[x], yhi[x], zlo[x], zhi[x]], axis=0)
        missing = jnp.dot(weights[:, cells:], around, preferred_element_type=jnp.float32)
        for weight, ref, at in outside:
            missing = missing + weight * ref[at].astype(jnp.float32)
        applied = inner[x] + missing * (1.0 / 24.0)
        top = applied.astype(jnp.bfloat16)
        rest = (applied - top.astype(jnp.float32)).astype(jnp.bfloat16)
        high[x] = top
        low[x] = rest

    outside = {
        0: ((1.0, xlo, 0), (-16.0, xlo, 1)),
        1: ((1.0, xlo, 1),),
        cx - 2: ((1.0, xhi, 0),),
        cx - 1: ((-16.0, xhi, 0), (1.0, xhi, 1)),
    }
    for x in range(cx):
        slab(x, outside.get(x, ()))
    flat = [ref[...].reshape(cx * cells, b) for ref in (p, high, low)]
    total = over_cells(jnp.concatenate(flat[:2], axis=1), jnp.concatenate(flat, axis=1))
    row, column = iotas(b, b)
    gram = total[:b, :b]
    cross = total[:b, b : 2 * b] + total[:b, 2 * b :]
    rest = total[b:, 2 * b :]
    square = total[b:, b : 2 * b] + rest + rest.T
    cross_own = jnp.sum(jnp.where(row == column, cross, 0.0), axis=0, keepdims=True)
    cross = cross + cross.T
    sums[:b] = jnp.where(row >= column, gram, cross)
    spare = jnp.where(row == 0, cross_own, pltpu.roll(jnp.broadcast_to(cross_own, (b, b)), b - 1, 1))
    sums[b:] = jnp.where(row > column, 2.0 * square, jnp.where(row == column, square, spare))


def across(value, lane):
    return jnp.take_along_axis(value, jnp.full(value.shape, lane, jnp.int32), axis=1)


def down(value, row):
    return jnp.broadcast_to(value[row : row + 1, :], value.shape)


def inverse_factor(rows):
    count = len(rows)
    size, bands = rows[0].shape
    row, column = iotas(size, bands)
    rows = list(rows)
    right = [jnp.where(column == row + size * k, 1.0, 0.0) for k in range(count)]
    done = []
    for k in range(count):
        lines = {
            i: [across(rows[i], size * k + c) for c in range(size)] for i in range(k, count)
        }
        own = lines.pop(k) + [rows[k], right[k]]
        result = jnp.zeros_like(right[k])
        for c in range(size):
            here = row == c
            pivot = down(own[c], c)
            scale = lax.rsqrt(pivot)
            share = 1.0 / pivot
            factor = jnp.where(here, -1.0, own[c])
            result = jnp.where(here, own[-1] * scale, result)
            for d in range(c + 1, len(own)):
                own[d] = jnp.where(here, 0.0, own[d]) - factor * (down(own[d], c) * share)
        done.append(result)
        heads = [(down(own[-2], c), down(own[-1], c)) for c in range(size)]
        for i, line in lines.items():
            for at in range(0, size, 2):
                rows[i] = rows[i] - (line[at] * heads[at][0] + line[at + 1] * heads[at + 1][0])
                right[i] = right[i] - (line[at] * heads[at][1] + line[at + 1] * heads[at + 1][1])
    return done


def split_3(value):
    parts = []
    for _ in range(3):
        part = value.astype(jnp.bfloat16)
        value = value - part.astype(jnp.float32)
        parts.append(part)
    return parts


def finish_kernel(
    cells, sums, p, high, low, rotated, residual, quotients, norms, w, out_r, out_s, sems
):
    bands = p.shape[1]
    row, column = iotas(bands, bands)
    scale = 1.0 / cells
    first, second = sums[:bands] * scale, sums[bands:] * scale
    lower = jnp.where(row >= column, first, 0.0)
    gram = lower + jnp.where(row > column, first, 0.0).T
    own = jnp.where(column[:1] == 0, pltpu.roll(second[:8], 1, 1)[1:2], second[:1])
    cross = jnp.where(row < column, first, jnp.where(row == column, own, 0.0))
    square = jnp.where(row >= column, second, 0.0)
    size = 16
    turned = jnp.concatenate(
        inverse_factor([gram[i : i + size] for i in range(0, bands, size)]), axis=0
    ).T
    none = jnp.zeros((bands, bands), jnp.bfloat16)
    for at, part in enumerate(split_3(turned)):
        w[at, :bands, :bands] = part
        w[at, :bands, bands:] = none
        w[at, bands:, :bands] = none
        w[at, bands:, bands:] = part if at < 2 else w[0, bands:, bands:]

    def diagonal(matrix):
        product = jnp.dot(matrix, turned, precision=HIGHEST, preferred_element_type=jnp.float32)
        return jnp.sum(product * turned, axis=0, keepdims=True)

    quotient = diagonal(cross)
    squares = diagonal(square) - quotient * quotient * (2.0 - diagonal(gram))
    quotients[...] = quotient
    norms[...] = jnp.sqrt(jnp.maximum(squares, 0.0) + 1e-06)
    copies = []
    start = 0
    for chunk, step in enumerate(CHUNKS):
        part = pl.ds(start, step)
        start += step
        both = jnp.concatenate([p[part], high[part]], axis=1)
        rest = jnp.concatenate([p[part], low[part]], axis=1)
        result = jnp.dot(rest, w[2], preferred_element_type=jnp.float32)
        result = result + jnp.dot(both, w[1], preferred_element_type=jnp.float32)
        result = result + jnp.dot(both, w[0], preferred_element_type=jnp.float32)
        bands_now = result[:, :bands]
        out_r[part] = bands_now
        out_s[part] = (result[:, bands:] - quotient * bands_now).astype(jnp.bfloat16)
        for at, (source, target) in enumerate(((out_r, rotated), (out_s, residual))):
            copy = pltpu.make_async_copy(source.at[part], target.at[part], sems.at[chunk, at])
            copy.start()
            copies.append(copy)
    for copy in copies:
        copy.wait()


def near(value):
    return pltpu.with_memory_space_constraint(value, pltpu.VMEM)


def far(value):
    return pltpu.with_memory_space_constraint(value, pltpu.HBM)


def from_below(edge, axes):
    count = lax.axis_size(axes)
    return lax.ppermute(edge, axes, [(i, (i + 1) % count) for i in range(count)])


def from_above(edge, axes):
    count = lax.axis_size(axes)
    return lax.ppermute(edge, axes, [((i + 1) % count, i) for i in range(count)])


def kernel_call(kernel, outs, ins, outs_at, scratch=(), **kept):
    return pl.pallas_call(
        kernel,
        out_shape=outs,
        in_specs=[pl.BlockSpec(memory_space=space) for space in ins],
        out_specs=tuple(pl.BlockSpec(memory_space=space) for space in outs_at),
        scratch_shapes=scratch,
        compiler_params=pltpu.CompilerParams(vmem_limit_bytes=VMEM_LIMIT),
        **kept,
    )


def exchange(blocks, axes):
    return lax.all_to_all(blocks, axes, split_axis=0, concat_axis=0, tiled=True)


def for_each(value, axes):
    return exchange(jnp.broadcast_to(value, (lax.axis_size(axes), *value.shape)), axes)


def sum_everywhere(value):
    rows, columns = value.shape
    own = jnp.sum(exchange(value.reshape(lax.axis_size(NEAR), -1, columns), NEAR), axis=0)
    own = jnp.sum(for_each(own, FAR), axis=0)
    return for_each(own, NEAR).reshape(rows, columns)


def local(wavefunctions, potential):
    cx, cy, cz, bands = wavefunctions.shape
    cells = cx * cy * cz
    total_cells = cells * lax.axis_size(GX) * lax.axis_size(GY) * lax.axis_size(GZ)
    planes = wavefunctions.reshape(cx, cy * cz, bands)
    weights = jnp.asarray(plane_weights(cy, cz), jnp.bfloat16)
    shape = planes.shape
    on_chip, off_chip = pltpu.VMEM, pltpu.HBM

    def half(*dims):
        return on_chip(dims, jnp.bfloat16)

    p, *edges, pot, w = kernel_call(
        functools.partial(prepare_kernel, cy),
        (
            half(*shape),
            *[half(2, cy * cz, bands)] * 2,
            *[half(cx, 2 * cz, bands)] * 2,
            *[half(cx, 2 * cy, bands)] * 2,
            on_chip(potential.shape, jnp.float32),
            half(*weights.shape),
        ),
        [off_chip] * 3,
        [on_chip] * 9,
        [pltpu.SemaphoreType.DMA((7,))],
        name="prepare",
    )(*map(far, (planes, potential, weights)))
    xlow, xhigh, ylow, yhigh, zlow, zhigh = edges
    xlo, xhi = from_below(xhigh, GX), from_above(xlow, GX)
    zlo, zhi = from_below(zhigh, GZ), from_above(zlow, GZ)
    ylo, yhi = from_below(yhigh, GY), from_above(ylow, GY)
    inner = kernel_call(
        inner_kernel, (on_chip(shape, jnp.float32),), [on_chip] * 3, [on_chip], name="inner"
    )(*map(near, (p, pot, w)))[0]
    high, low, sums = kernel_call(
        apply_kernel,
        (half(*shape), half(*shape), on_chip((2 * bands, bands), jnp.float32)),
        [on_chip] * 9,
        [on_chip] * 3,
        name="apply",
    )(*map(near, (p, inner, xlo, xhi, zlo, zhi, ylo, yhi, w)))
    sums = sum_everywhere(sums)
    flat = (cells, bands)
    line = jax.ShapeDtypeStruct((1, bands), jnp.float32)
    rotated, residual, quotients, norms = kernel_call(
        functools.partial(finish_kernel, total_cells),
        (
            jax.ShapeDtypeStruct(flat, jnp.float32),
            jax.ShapeDtypeStruct(flat, jnp.bfloat16),
            line,
            line,
        ),
        [on_chip] * 4,
        [off_chip, off_chip, on_chip, on_chip],
        [
            pltpu.VMEM((3, 2 * bands, 2 * bands), jnp.bfloat16),
            pltpu.VMEM(flat, jnp.float32),
            pltpu.VMEM(flat, jnp.bfloat16),
            pltpu.SemaphoreType.DMA((len(CHUNKS), 2)),
        ],
        name="finish",
    )(*map(near, (sums, p.reshape(flat), high.reshape(flat), low.reshape(flat))))
    whole = (cx, cy, cz, bands)
    return rotated.reshape(whole), residual.reshape(whole), quotients[0], norms[0]


def solution(mesh):
    count = mesh.shape
    torus = Mesh(
        mesh.devices.reshape(count["gx"] // 2, 2, count["gy"] // 2, 2, count["gz"] // 2, 2),
        GX + GY + GZ,
    )
    return jax.shard_map(
        local,
        mesh=torus,
        in_specs=(P(GX, GY, GZ, None), P(GX, GY, GZ)),
        out_specs=(P(GX, GY, GZ, None), P(GX, GY, GZ, None), P(), P()),
        check_vma=False,
    )
```

```python
import functools

import jax
import jax.numpy as jnp
import numpy as np
from jax import lax
from jax.experimental import pallas as pl
from jax.experimental.pallas import tpu as pltpu
from jax.sharding import Mesh
from jax.sharding import PartitionSpec as P

GX = ("gx_0", "gx_1")
GY = ("gy_0", "gy_1")
GZ = ("gz_0", "gz_1")
NEAR = ("gz_1", "gx_1", "gy_1", "gy_0")
FAR = ("gz_0", "gx_0")
HIGHEST = lax.Precision.HIGHEST
CHUNKS = (512,) * 8
VMEM_LIMIT = 24 * 2**20


def plane_weights(cy, cz):
    side = {0: 90.0, 1: -16.0, 2: 1.0}
    weights = np.zeros((cy * cz, cy * cz + 4 * cz + 4 * cy), np.float32)
    for y in range(cy):
        for z in range(cz):
            row = y * cz + z
            weights[row, row] = side[0]
            for step in (-2, -1, 1, 2):
                w = side[abs(step)]
                base = cy * cz
                if 0 <= y + step < cy:
                    weights[row, row + step * cz] = w
                elif y + step < 0:
                    weights[row, base + (y + step + 2) * cz + z] = w
                else:
                    weights[row, base + 2 * cz + (y + step - cy) * cz + z] = w
                base = cy * cz + 4 * cz
                if 0 <= z + step < cz:
                    weights[row, row + step] = w
                elif z + step < 0:
                    weights[row, base + y * 2 + z + step + 2] = w
                else:
                    weights[row, base + 2 * cy + y * 2 + z + step - cz] = w
    return weights


def over_cells(left, right):
    return lax.dot_general(
        left, right, (((0,), (0,)), ((), ())), preferred_element_type=jnp.float32
    )


def iotas(rows, columns):
    shape = (rows, columns)
    return lax.broadcasted_iota(jnp.int32, shape, 0), lax.broadcasted_iota(jnp.int32, shape, 1)


def prepare_kernel(cy, given, potential, weights, p, xlo, xhi, ylo, yhi, zlo, zhi, pot, w, sems):
    cx, cells, bands = p.shape
    cz = cells // cy
    edge = 2 * cz
    pairs = (
        (given, p),
        (given.at[:2], xlo),
        (given.at[cx - 2 :], xhi),
        (given.at[:, :edge], ylo),
        (given.at[:, cells - edge :], yhi),
        (potential, pot),
        (weights, w),
    )
    copies = [pltpu.make_async_copy(*pair, sems.at[at]) for at, pair in enumerate(pairs)]
    for copy in copies:
        copy.start()
    row, column = iotas(4 * cy, cells)
    side, row = row // (2 * cy), row % (2 * cy)
    source = (row // 2) * cz + row % 2 + side * (cz - 2)
    choice = jnp.where(column == source, 1.0, 0.0).astype(jnp.bfloat16)
    copies[0].wait()
    for x in range(cx):
        faces = jnp.dot(choice, p[x], preferred_element_type=jnp.float32).astype(jnp.bfloat16)
        zlo[x] = faces[: 2 * cy]
        zhi[x] = faces[2 * cy :]
    for copy in copies[1:]:
        copy.wait()


def inner_kernel(p, pot, weights, inner):
    cx, cells, bands = p.shape
    cy, cz = pot.shape[1:]

    def slab(x, steps):
        own = p[x]
        total = jnp.dot(weights[:, :cells], own, preferred_element_type=jnp.float32)
        for step in steps:
            near_by = p[x + step].astype(jnp.float32)
            total = total + near_by if abs(step) == 2 else total - 16.0 * near_by
        lines = pot[x].T
        given = jnp.concatenate(
            [jnp.broadcast_to(lines[:, y : y + 1], (cz, bands)) for y in range(cy)], axis=0
        ) * own.astype(jnp.float32)
        inner[x] = total * (1.0 / 24.0) + given

    for x in range(cx):
        slab(x, [step for step in (-2, -1, 1, 2) if 0 <= x + step < cx])


def apply_kernel(p, inner, xlo, xhi, zlo, zhi, ylo, yhi, weights, high, low, sums):
    cx, cells, bands = p.shape
    b = bands

    def slab(x, outside=()):
        around = jnp.concatenate([ylo[x], yhi[x], zlo[x], zhi[x]], axis=0)
        missing = jnp.dot(weights[:, cells:], around, preferred_element_type=jnp.float32)
        for weight, ref, at in outside:
            missing = missing + weight * ref[at].astype(jnp.float32)
        applied = inner[x] + missing * (1.0 / 24.0)
        top = applied.astype(jnp.bfloat16)
        rest = (applied - top.astype(jnp.float32)).astype(jnp.bfloat16)
        high[x] = top
        low[x] = rest

    outside = {
        0: ((1.0, xlo, 0), (-16.0, xlo, 1)),
        1: ((1.0, xlo, 1),),
        cx - 2: ((1.0, xhi, 0),),
        cx - 1: ((-16.0, xhi, 0), (1.0, xhi, 1)),
    }
    for x in range(cx):
        slab(x, outside.get(x, ()))
    flat = [ref[...].reshape(cx * cells, b) for ref in (p, high, low)]
    total = over_cells(jnp.concatenate(flat[:2], axis=1), jnp.concatenate(flat, axis=1))
    row, column = iotas(b, b)
    gram = total[:b, :b]
    cross = total[:b, b : 2 * b] + total[:b, 2 * b :]
    rest = total[b:, 2 * b :]
    square = total[b:, b : 2 * b] + rest + rest.T
    cross_own = jnp.sum(jnp.where(row == column, cross, 0.0), axis=0, keepdims=True)
    cross = cross + cross.T
    sums[:b] = jnp.where(row >= column, gram, cross)
    spare = jnp.where(row == 0, cross_own, pltpu.roll(jnp.broadcast_to(cross_own, (b, b)), b - 1, 1))
    sums[b:] = jnp.where(row > column, 2.0 * square, jnp.where(row == column, square, spare))


def across(value, lane):
    return jnp.take_along_axis(value, jnp.full(value.shape, lane, jnp.int32), axis=1)


def down(value, row):
    return jnp.broadcast_to(value[row : row + 1, :], value.shape)


def inverse_factor(rows):
    count = len(rows)
    size, bands = rows[0].shape
    row, column = iotas(size, bands)
    rows = list(rows)
    right = [jnp.where(column == row + size * k, 1.0, 0.0) for k in range(count)]
    done = []
    for k in range(count):
        lines = {
            i: [across(rows[i], size * k + c) for c in range(size)] for i in range(k, count)
        }
        own = lines.pop(k) + [rows[k], right[k]]
        result = jnp.zeros_like(right[k])
        for c in range(size):
            here = row == c
            pivot = down(own[c], c)
            scale = lax.rsqrt(pivot)
            share = 1.0 / pivot
            factor = jnp.where(here, -1.0, own[c])
            result = jnp.where(here, own[-1] * scale, result)
            for d in range(c + 1, len(own)):
                own[d] = jnp.where(here, 0.0, own[d]) - factor * (down(own[d], c) * share)
        done.append(result)
        heads = [(down(own[-2], c), down(own[-1], c)) for c in range(size)]
        for i, line in lines.items():
            for at in range(0, size, 2):
                rows[i] = rows[i] - (line[at] * heads[at][0] + line[at + 1] * heads[at + 1][0])
                right[i] = right[i] - (line[at] * heads[at][1] + line[at + 1] * heads[at + 1][1])
    return done


def split_3(value):
    parts = []
    for _ in range(3):
        part = value.astype(jnp.bfloat16)
        value = value - part.astype(jnp.float32)
        parts.append(part)
    return parts


def finish_kernel(
    cells, sums, p, high, low, rotated, residual, quotients, norms, w, out_r, out_s, sems
):
    bands = p.shape[1]
    row, column = iotas(bands, bands)
    scale = 1.0 / cells
    first, second = sums[:bands] * scale, sums[bands:] * scale
    lower = jnp.where(row >= column, first, 0.0)
    gram = lower + jnp.where(row > column, first, 0.0).T
    own = jnp.where(column[:1] == 0, pltpu.roll(second[:8], 1, 1)[1:2], second[:1])
    cross = jnp.where(row < column, first, jnp.where(row == column, own, 0.0))
    square = jnp.where(row >= column, second, 0.0)
    size = 16
    turned = jnp.concatenate(
        inverse_factor([gram[i : i + size] for i in range(0, bands, size)]), axis=0
    ).T
    none = jnp.zeros((bands, bands), jnp.bfloat16)
    for at, part in enumerate(split_3(turned)):
        w[at, :bands, :bands] = part
        w[at, :bands, bands:] = none
        w[at, bands:, :bands] = none
        w[at, bands:, bands:] = part if at < 2 else w[0, bands:, bands:]

    product = jnp.dot(
        jnp.concatenate([cross, square, gram], axis=0),
        turned,
        precision=HIGHEST,
        preferred_element_type=jnp.float32,
    )
    quotient, applied_square, rotated_square = (
        jnp.sum(product[i : i + bands] * turned, axis=0, keepdims=True)
        for i in range(0, 3 * bands, bands)
    )
    squares = applied_square - quotient * quotient * (2.0 - rotated_square)
    quotients[...] = quotient
    norms[...] = jnp.sqrt(jnp.maximum(squares, 0.0) + 1e-06)
    copies = []
    start = 0
    for chunk, step in enumerate(CHUNKS):
        part = pl.ds(start, step)
        start += step
        both = jnp.concatenate([p[part], high[part]], axis=1)
        rest = jnp.concatenate([p[part], low[part]], axis=1)
        result = jnp.dot(rest, w[2], preferred_element_type=jnp.float32)
        result = result + jnp.dot(both, w[1], preferred_element_type=jnp.float32)
        result = result + jnp.dot(both, w[0], preferred_element_type=jnp.float32)
        bands_now = result[:, :bands]
        out_r[part] = bands_now
        out_s[part] = (result[:, bands:] - quotient * bands_now).astype(jnp.bfloat16)
        for at, (source, target) in enumerate(((out_r, rotated), (out_s, residual))):
            copy = pltpu.make_async_copy(source.at[part], target.at[part], sems.at[chunk, at])
            copy.start()
            copies.append(copy)
    for copy in copies:
        copy.wait()


def near(value):
    return pltpu.with_memory_space_constraint(value, pltpu.VMEM)


def far(value):
    return pltpu.with_memory_space_constraint(value, pltpu.HBM)


def from_below(edge, axes):
    count = lax.axis_size(axes)
    return lax.ppermute(edge, axes, [(i, (i + 1) % count) for i in range(count)])


def from_above(edge, axes):
    count = lax.axis_size(axes)
    return lax.ppermute(edge, axes, [((i + 1) % count, i) for i in range(count)])


def kernel_call(kernel, outs, ins, outs_at, scratch=(), **kept):
    return pl.pallas_call(
        kernel,
        out_shape=outs,
        in_specs=[pl.BlockSpec(memory_space=space) for space in ins],
        out_specs=tuple(pl.BlockSpec(memory_space=space) for space in outs_at),
        scratch_shapes=scratch,
        compiler_params=pltpu.CompilerParams(vmem_limit_bytes=VMEM_LIMIT),
        **kept,
    )


def exchange(blocks, axes):
    return lax.all_to_all(blocks, axes, split_axis=0, concat_axis=0, tiled=True)


def for_each(value, axes):
    return exchange(jnp.broadcast_to(value, (lax.axis_size(axes), *value.shape)), axes)


def sum_everywhere(value):
    rows, columns = value.shape
    own = jnp.sum(exchange(value.reshape(lax.axis_size(NEAR), -1, columns), NEAR), axis=0)
    own = jnp.sum(for_each(own, FAR), axis=0)
    return for_each(own, NEAR).reshape(rows, columns)


def local(wavefunctions, potential):
    cx, cy, cz, bands = wavefunctions.shape
    cells = cx * cy * cz
    total_cells = cells * lax.axis_size(GX) * lax.axis_size(GY) * lax.axis_size(GZ)
    planes = wavefunctions.reshape(cx, cy * cz, bands)
    weights = jnp.asarray(plane_weights(cy, cz), jnp.bfloat16)
    shape = planes.shape
    on_chip, off_chip = pltpu.VMEM, pltpu.HBM

    def half(*dims):
        return on_chip(dims, jnp.bfloat16)

    p, *edges, pot, w = kernel_call(
        functools.partial(prepare_kernel, cy),
        (
            half(*shape),
            *[half(2, cy * cz, bands)] * 2,
            *[half(cx, 2 * cz, bands)] * 2,
            *[half(cx, 2 * cy, bands)] * 2,
            on_chip(potential.shape, jnp.float32),
            half(*weights.shape),
        ),
        [off_chip] * 3,
        [on_chip] * 9,
        [pltpu.SemaphoreType.DMA((7,))],
        name="prepare",
    )(*map(far, (planes, potential, weights)))
    xlow, xhigh, ylow, yhigh, zlow, zhigh = edges
    xlo, xhi = from_below(xhigh, GX), from_above(xlow, GX)
    zlo, zhi = from_below(zhigh, GZ), from_above(zlow, GZ)
    ylo, yhi = from_below(yhigh, GY), from_above(ylow, GY)
    inner = kernel_call(
        inner_kernel, (on_chip(shape, jnp.float32),), [on_chip] * 3, [on_chip], name="inner"
    )(*map(near, (p, pot, w)))[0]
    high, low, sums = kernel_call(
        apply_kernel,
        (half(*shape), half(*shape), on_chip((2 * bands, bands), jnp.float32)),
        [on_chip] * 9,
        [on_chip] * 3,
        name="apply",
    )(*map(near, (p, inner, xlo, xhi, zlo, zhi, ylo, yhi, w)))
    sums = sum_everywhere(sums)
    flat = (cells, bands)
    line = jax.ShapeDtypeStruct((1, bands), jnp.float32)
    rotated, residual, quotients, norms = kernel_call(
        functools.partial(finish_kernel, total_cells),
        (
            jax.ShapeDtypeStruct(flat, jnp.float32),
            jax.ShapeDtypeStruct(flat, jnp.bfloat16),
            line,
            line,
        ),
        [on_chip] * 4,
        [off_chip, off_chip, on_chip, on_chip],
        [
            pltpu.VMEM((3, 2 * bands, 2 * bands), jnp.bfloat16),
            pltpu.VMEM(flat, jnp.float32),
            pltpu.VMEM(flat, jnp.bfloat16),
            pltpu.SemaphoreType.DMA((len(CHUNKS), 2)),
        ],
        name="finish",
    )(*map(near, (sums, p.reshape(flat), high.reshape(flat), low.reshape(flat))))
    whole = (cx, cy, cz, bands)
    return rotated.reshape(whole), residual.reshape(whole), quotients[0], norms[0]


def solution(mesh):
    count = mesh.shape
    torus = Mesh(
        mesh.devices.reshape(count["gx"] // 2, 2, count["gy"] // 2, 2, count["gz"] // 2, 2),
        GX + GY + GZ,
    )
    return jax.shard_map(
        local,
        mesh=torus,
        in_specs=(P(GX, GY, GZ, None), P(GX, GY, GZ)),
        out_specs=(P(GX, GY, GZ, None), P(GX, GY, GZ, None), P(), P()),
        check_vma=False,
    )
```
